32 devices in a mesh: slab: 4 (over z), tile: 8 (over y, x, core).
Axes of the slice: x: 2, y: 2, z: 4, core: 2. Of those that a mesh axis runs over, the one named last changes fastest.
Arguments:
- voxel_grid: float32 [4, 64, 64, 256], P(None, 'slab', 'tile'), may hold values from -4 to 4
- first_moment: float32 [4, 64, 64, 256], P(None, 'slab', 'tile'), may hold values from -0.75 to 0.75
- second_moment: float32 [4, 64, 64, 256], P(None, 'slab', 'tile'), may hold values from 0.01 to 0.5
- pixel_index: int32 [32768], P('tile'), may hold values from 0 to 2047
- start_slab: int32 [32768], P('tile'), may hold values from 0 to 1
- ray_count: int32 [32768], P('tile'), may hold values from 16 to 48
- target: float32 [3, 32768], P(None, 'tile'), may hold values from 0 to 1
Outputs:
- new_grid: float32 [4, 64, 64, 256], P(None, 'slab', 'tile')
- new_first: float32 [4, 64, 64, 256], P(None, 'slab', 'tile')
- new_second: float32 [4, 64, 64, 256], P(None, 'slab', 'tile')
The draws below stay inside these ranges and needn't reach their ends.
All inputs are finite; a program needn't handle non-finite values.
Results may differ from the reference program's by a relative error of at most 0.0003.
Values sent between devices are 32-bit elements; how exact they have to be, the bound alone decides.
No kernel may reach another device: no remote copies, remote signals or barrier semaphores. Data moves between devices by JAX's collectives and lax.ppermute only.
A program may use at most 128 MiB of HBM per device.

```python
import math
import jax
import jax.numpy as jnp
from jax import lax

CZ = 16
CX = 8
NY = 256
RAYS_DEV = 4096
STEP = 20
NZ = 64
NX = 64
RAYS = 32768
HALF_SLABS = 2
N_TILE = 8


def place_ends(result, rng, least, top_value):
    longest = result.shape.index(max(result.shape))
    spots = []
    for shift in (0, 1):
        where = [jax.random.randint(jax.random.fold_in(rng, axis), (), 0, length) for axis, length in enumerate(result.shape)]
        where[longest] = (where[longest] + shift) % result.shape[longest]
        spots.append(tuple(where))
    return result.at[spots[0]].set(least).at[spots[1]].set(top_value)


def block_levels(key, shape, pieces, least, top_value):
    loudness = 1.0
    for axis_at, blocks in pieces:
        draws = jax.random.uniform(jax.random.fold_in(jax.random.fold_in(key, 6), axis_at), (blocks,), jnp.float32, least / len(pieces), top_value / len(pieces))
        loudness = loudness * jnp.repeat(jnp.exp(draws), shape[axis_at] // blocks).reshape((-1,) + (1,) * (len(shape) - 1 - axis_at))
    return loudness


def bell_draw(key, dims, spread, reach, split=(), kind=jnp.bfloat16):
    array = spread * jax.random.normal(key, dims, jnp.float32)
    if split:
        array = array * block_levels(key, dims, split, -0.22, 0.18)
    return jnp.clip(array, -reach, reach).astype(kind)


def setup_inputs(seed: int = 0) -> dict:
    seeds = jax.random.split(jax.random.key(seed), 8)
    return {
        "voxel_grid": bell_draw(seeds[0], (4, NZ, NX, NY), 1.0, 4.0, ((1, 4), (2, 8)), jnp.float32),
        "first_moment": bell_draw(seeds[1], (4, NZ, NX, NY), 0.05, 0.75, ((1, 4), (2, 8)), jnp.float32),
        "second_moment": jnp.clip(jnp.exp(math.log(0.5) - 3.912023 * jax.random.uniform(seeds[2], (4, NZ, NX, NY), jnp.float32) ** block_levels(seeds[2], (4, NZ, NX, NY), ((1, 4), (2, 8)), -0.2, 0.2)), 0.01, 0.5),
        "pixel_index": place_ends(jax.random.randint(seeds[3], (RAYS,), 0, CX * NY), jax.random.fold_in(seeds[3], 1), 0, (CX * NY) - 1).astype(jnp.int32),
        "start_slab": place_ends(jax.random.randint(seeds[4], (RAYS,), 0, HALF_SLABS), jax.random.fold_in(seeds[4], 1), 0, HALF_SLABS - 1).astype(jnp.int32),
        "ray_count": place_ends(jax.random.randint(seeds[5], (RAYS,), NZ // 4, NZ // 2 + CZ + 1), jax.random.fold_in(seeds[5], 1), NZ // 4, (NZ // 2 + CZ + 1) - 1).astype(jnp.int32),
        "target": jnp.clip(1.0 * jax.random.uniform(seeds[6], (3, RAYS), jnp.float32) ** block_levels(seeds[6], (3, RAYS), ((1, 8),), -0.2, 0.2), 0.0, 1.0),
    }


RENDER_WEIGHT = 1000.0
TV_WEIGHT = 0.05
BACKGROUND = 1.0
STEP_SPAN = 4.0
CLIP_RMS = 0.25
LEARN_RATE = 0.02
BETA_ONE = 0.9
BETA_TWO = 0.99
EPSILON = 1e-08

def tile_loss(tile_grid, pixel_index, start_slab, ray_count, target):
    flat = tile_grid.reshape(4, NZ, CX * NY)
    samples = jnp.take(flat, pixel_index, axis=2)
    depth_pos = jnp.arange(NZ, dtype=jnp.int32)[:, None]
    first_cell = start_slab[None, :] * CZ
    inside = (depth_pos >= first_cell) & (depth_pos < first_cell + ray_count[None, :])
    optical = jnp.where(inside, jax.nn.softplus(samples[0]) * (STEP_SPAN / NZ), 0.0)
    running = jnp.cumsum(optical, axis=0)
    weights = jnp.exp(-(running - optical)) * (1.0 - jnp.exp(-optical))
    colors = jax.nn.sigmoid(samples[1:4])
    rendered = lax.optimization_barrier(jnp.sum(weights[None] * colors, axis=1)) + jnp.exp(-running[-1])[None] * BACKGROUND
    return 0.5 * RENDER_WEIGHT * jnp.sum((rendered - target) ** 2)

def reference(voxel_grid, first_moment, second_moment, pixel_index, start_slab, ray_count, target):
    tiles = voxel_grid.reshape(4, NZ, N_TILE, CX, NY).transpose(2, 0, 1, 3, 4)
    pixels = pixel_index.reshape(N_TILE, RAYS_DEV)
    starts = start_slab.reshape(N_TILE, RAYS_DEV)
    counts = ray_count.reshape(N_TILE, RAYS_DEV)
    targets = target.reshape(3, N_TILE, RAYS_DEV).transpose(1, 0, 2)

    def one_tile(inputs):
        return jax.grad(tile_loss)(*inputs)
    tile_grads = lax.map(one_tile, (tiles, pixels, starts, counts, targets))
    render_grad = tile_grads.transpose(1, 2, 0, 3, 4).reshape(4, NZ, NX, NY)
    smooth = jnp.zeros_like(voxel_grid)
    for axis_num in (1, 2, 3):
        step_diff = jnp.diff(voxel_grid, axis=axis_num)
        low_pad = [(0, 0)] * 4
        high_pad = [(0, 0)] * 4
        low_pad[axis_num] = (0, 1)
        high_pad[axis_num] = (1, 0)
        smooth = smooth + jnp.pad(-step_diff, low_pad) + jnp.pad(step_diff, high_pad)
    gradient = render_grad + 2.0 * TV_WEIGHT * smooth
    norm_value = jnp.sqrt(jnp.sum(gradient * gradient))
    limit = CLIP_RMS * math.sqrt(4.0 * NZ * NX * NY)
    clipped = gradient * (limit / jnp.maximum(norm_value, limit))
    new_first = BETA_ONE * first_moment + (1.0 - BETA_ONE) * clipped
    new_second = BETA_TWO * second_moment + (1.0 - BETA_TWO) * clipped * clipped
    first_hat = new_first / (1.0 - BETA_ONE ** STEP)
    second_hat = new_second / (1.0 - BETA_TWO ** STEP)
    new_grid = voxel_grid - LEARN_RATE * first_hat / (jnp.sqrt(second_hat) + EPSILON)
    return (new_grid, new_first, new_second)
```

```python
import math

import jax
import jax.numpy as jnp
from jax import lax
from jax.experimental import pallas as pl
from jax.experimental.pallas import tpu as pltpu
from jax.sharding import PartitionSpec as P

STEP = 20


RENDER_WEIGHT = 1000.0
TV_WEIGHT = 0.05
BACKGROUND = 1.0
STEP_SPAN = 4.0
CLIP_RMS = 0.25
LEARN_RATE = 0.02
BETA_ONE = 0.9
BETA_TWO = 0.99
EPSILON = 1e-08
BLOCK_LIMIT = 1024


def split_bf16(value):
    high = value.astype(jnp.bfloat16)
    low = (value - high.astype(jnp.float32)).astype(jnp.bfloat16)
    return high, low


def softplus(value):
    return jnp.maximum(value, 0.0) + jnp.log1p(jnp.exp(-jnp.abs(value)))


def ray_keys(pixel, start, count, slab_pos, depth, rows_x, rows_y):
    shift = rows_y.bit_length() - 1
    x = jnp.right_shift(pixel, shift)
    y = jnp.bitwise_and(pixel, rows_y - 1)
    first = (start - slab_pos) * depth
    used = jnp.clip(first + count, 0, depth)
    key = jnp.where((first <= 0) & (used > 0), (used - 1) * rows_x + x, -1)
    return y, key


def one_hot(y, rows_y):
    ids = lax.broadcasted_iota(jnp.int32, (rows_y, y.shape[1]), 0)
    return jnp.where(ids == y, 1.0, 0.0).astype(jnp.bfloat16)


def forward_kernel(total_depth, grid, pixel, start, count, part, to_next, to_prev, table):
    channels, depth, rows_x, rows_y = grid.shape
    rows = depth * rows_x
    rays = pixel.shape[1]
    half = rays // 2
    slab_pos = lax.axis_index("slab")
    reach = jnp.ones((rows_x, rows_y), jnp.float32)
    sums = [jnp.zeros((rows_x, rows_y), jnp.float32) for _ in range(3)]
    held = []
    for z in range(depth):
        fade = jnp.exp(-softplus(grid[0, z]) * (STEP_SPAN / total_depth))
        weight = reach * (1.0 - fade)
        reach = reach * fade
        sums = [sums[c] + weight * lax.logistic(grid[c + 1, z]) for c in range(3)]
        held.append(sums + [reach])
        if z % 2:
            for c in range(4):
                high, low = split_bf16(jnp.concatenate([held[0][c], held[1][c]], axis=0))
                at = c * rows + (z - 1) * rows_x
                table[at : at + 2 * rows_x, :rows_y] = high
                table[at : at + 2 * rows_x, rows_y:] = low
            held = []
    block = math.gcd(half, 512)
    for at in range(0, rays, block):
        where = slice(at, at + block)
        y, key = ray_keys(
            pixel[:, where], start[:, where], count[:, where], slab_pos, depth, rows_x, rows_y
        )
        hot = one_hot(y, rows_y)
        picked = jnp.dot(
            table[...], jnp.concatenate([hot, hot], axis=0), preferred_element_type=jnp.float32
        )
        match = lax.broadcasted_iota(jnp.int32, (rows, block), 0) == key
        found = [
            jnp.sum(
                jnp.where(match, picked[c * rows : (c + 1) * rows], 0.0), axis=0, keepdims=True
            )
            for c in range(4)
        ]
        found[3] = jnp.where(key < 0, 1.0, found[3])
        found = jnp.concatenate(found, axis=0)
        row = 4 * (at // half)
        lane = at % half
        for out in (part, to_next, to_prev):
            out[row : row + 4, lane : lane + block] = found
    for c in range(channels):
        at = half + c * rows_y
        to_next[:, at : at + rows_y] = grid[c, depth - 1]
        to_prev[:, at : at + rows_y] = grid[c, 0]


def backward_kernel(
    slab_count, tile_count, grid, pixel, start, count, target, x_low, x_high, part, *rest
):
    others = rest[: slab_count - 1]
    gradient, square, left, right, spread = rest[slab_count - 1 :]
    channels, depth, rows_x, rows_y = grid.shape
    rows = depth * rows_x
    rays = pixel.shape[1]
    half = rays // 2
    total_depth = depth * slab_count
    slab_pos = lax.axis_index("slab")
    tile_pos = lax.axis_index("tile")
    block = math.gcd(half, 1024)
    for at in range(0, rays, block):
        where = slice(at, at + block)
        row = 4 * (at // half)
        lanes = slice(at % half, at % half + block)

        def piece(ref):
            return ref[row : row + 3, lanes], ref[row + 3 : row + 4, lanes]

        front_color = jnp.zeros((3, block), jnp.float32)
        front_trans = jnp.ones((1, block), jnp.float32)
        beyond = jnp.full((3, block), BACKGROUND, jnp.float32)
        for k in range(slab_count - 1, 0, -1):
            color, trans = piece(others[k - 1])
            nearer = slab_pos >= k
            front_color = jnp.where(nearer, front_color + front_trans * color, front_color)
            front_trans = jnp.where(nearer, front_trans * trans, front_trans)
            color, trans = piece(others[slab_count - k - 1])
            farther = slab_pos + k < slab_count
            beyond = jnp.where(farther, color + trans * beyond, beyond)
        own_color, own_trans = piece(part)
        rendered = front_color + front_trans * (own_color + own_trans * beyond)
        residual = RENDER_WEIGHT * (rendered - target[:, where])
        color_cot = front_trans * residual
        trans_cot = front_trans * jnp.sum(residual * beyond, axis=0, keepdims=True)
        y, key = ray_keys(
            pixel[:, where], start[:, where], count[:, where], slab_pos, depth, rows_x, rows_y
        )
        hot = one_hot(y, rows_y)
        match = lax.broadcasted_iota(jnp.int32, (rows, block), 0) == key
        for c in range(4):
            cot = color_cot[c : c + 1] if c < 3 else trans_cot
            high = cot.astype(jnp.bfloat16).astype(jnp.float32)
            low = cot - high
            for j, value in enumerate((high, low)):
                left[c * rows : (c + 1) * rows, j * block : (j + 1) * block] = jnp.where(
                    match, value, 0.0
                ).astype(jnp.bfloat16)
        for j in range(2):
            right[:, j * block : (j + 1) * block] = hot
        added = lax.dot_general(
            left[...], right[...], (((1,), (1,)), ((), ())), preferred_element_type=jnp.float32
        )
        if at == 0:
            spread[...] = added
        else:
            spread[...] += added

    reach = [jnp.ones((rows_x, rows_y), jnp.float32)]
    fades = []
    for z in range(depth):
        fades.append(jnp.exp(-softplus(grid[0, z]) * (STEP_SPAN / total_depth)))
        reach.append(reach[z] * fades[z])
    row_ids = lax.broadcasted_iota(jnp.int32, (rows_x, rows_y), 0)
    lane_ids = lax.broadcasted_iota(jnp.int32, (rows_x, rows_y), 1)
    has_low = (row_ids > 0) | (tile_pos > 0)
    has_high = (row_ids < rows_x - 1) | (tile_pos < tile_count - 1)
    total = jnp.zeros((rows_x, rows_y), jnp.float32)

    def smooth(c, z):
        value = grid[c, z]
        lanes = slice(half + c * rows_y, half + (c + 1) * rows_y)
        if z > 0:
            out = value - grid[c, z - 1]
        else:
            out = jnp.where(slab_pos > 0, value - others[0][:, lanes], 0.0)
        if z < depth - 1:
            out = out + (value - grid[c, z + 1])
        else:
            out = out + jnp.where(
                slab_pos < slab_count - 1, value - others[slab_count - 2][:, lanes], 0.0
            )
        at = c * depth + z
        low = jnp.where(row_ids == 0, x_low[at : at + 1], pltpu.roll(value, 1, 0))
        high = jnp.where(
            row_ids == rows_x - 1, x_high[at : at + 1], pltpu.roll(value, rows_x - 1, 0)
        )
        out = out + jnp.where(has_low, value - low, 0.0) + jnp.where(has_high, value - high, 0.0)
        out = out + jnp.where(lane_ids > 0, value - pltpu.roll(value, 1, 1), 0.0)
        out = out + jnp.where(
            lane_ids < rows_y - 1, value - pltpu.roll(value, rows_y - 1, 1), 0.0
        )
        return (2.0 * TV_WEIGHT) * out

    below = [jnp.zeros((rows_x, rows_y), jnp.float32) for _ in range(3)]
    gain_after = jnp.zeros((rows_x, rows_y), jnp.float32)
    tail = jnp.zeros((rows_x, rows_y), jnp.float32)
    for z in range(depth - 1, -1, -1):
        rate = 1.0 - fades[z]
        weight = reach[z] * rate
        gain = jnp.zeros((rows_x, rows_y), jnp.float32)
        for c in range(3):
            at = c * rows + z * rows_x
            below[c] = below[c] + spread[at : at + rows_x]
            shade = lax.logistic(grid[c + 1, z])
            gain = gain + shade * below[c]
            value = weight * below[c] * shade * (1.0 - shade) + smooth(c + 1, z)
            gradient[c + 1, z] = value
            total = total + value * value
        at = 3 * rows + z * rows_x
        tail = tail + reach[z + 1] * (gain_after - gain + spread[at : at + rows_x])
        value = smooth(0, z) - tail * (STEP_SPAN / total_depth) * lax.logistic(grid[0, z])
        gradient[0, z] = value
        total = total + value * value
        gain_after = gain
    square[...] = jnp.broadcast_to(jnp.sum(total).reshape(1, 1), square.shape)


def group_sum(value, axis, masks):
    count = lax.axis_size(axis)
    parts = [lax.ppermute(value, axis, [(i, i ^ m) for i in range(count)]) for m in masks]
    for part in parts:
        value = value + part
    return value


def global_sum(value):
    for axis in ("slab", "tile"):
        left = lax.axis_size(axis)
        base = 1
        rounds = []
        if axis == "tile":
            rounds.append([1])
            base = 2
        while base < left:
            if base * 4 <= left:
                rounds.append([base, 2 * base, 3 * base])
                base *= 4
            else:
                rounds.append([base])
                base *= 2
        for masks in reversed(rounds):
            value = group_sum(value, axis, masks)
    return value


def per_device(voxel_grid, first_moment, second_moment, pixel_index, start_slab, ray_count, target):
    slab_count = lax.axis_size("slab")
    tile_count = lax.axis_size("tile")
    channels, depth, rows_x, rows_y = voxel_grid.shape
    total_depth = depth * slab_count
    total_x = rows_x * tile_count
    rays = pixel_index.shape[0]
    half = rays // 2
    f32 = jnp.float32
    pixel = pixel_index.reshape(1, rays)
    start = start_slab.reshape(1, rays)
    count = ray_count.reshape(1, rays)
    first_rows = voxel_grid[:, :, 0, :].reshape(channels * depth, rows_y)
    last_rows = voxel_grid[:, :, rows_x - 1, :].reshape(channels * depth, rows_y)
    x_low = lax.ppermute(last_rows, "tile", [(i, i + 1) for i in range(tile_count - 1)])
    x_high = lax.ppermute(first_rows, "tile", [(i + 1, i) for i in range(tile_count - 1)])
    wide = jax.ShapeDtypeStruct((8, half + channels * rows_y), f32)
    part, to_next, to_prev = pl.pallas_call(
        lambda *refs: forward_kernel(total_depth, *refs),
        out_shape=(jax.ShapeDtypeStruct((8, half), f32), wide, wide),
        scratch_shapes=[pltpu.VMEM((4 * depth * rows_x, 2 * rows_y), jnp.bfloat16)],
        name="forward",
    )(voxel_grid, pixel, start, count)
    others = []
    for k in range(1, slab_count):
        sent = to_next if k == 1 else to_prev if k == slab_count - 1 else part
        others.append(
            lax.ppermute(sent, "slab", [(i, (i + k) % slab_count) for i in range(slab_count)])
        )
    block = math.gcd(half, 1024)
    gradient, square = pl.pallas_call(
        lambda *refs: backward_kernel(slab_count, tile_count, *refs),
        out_shape=(
            jax.ShapeDtypeStruct(voxel_grid.shape, f32),
            jax.ShapeDtypeStruct((1, 128), f32),
        ),
        scratch_shapes=[
            pltpu.VMEM((4 * depth * rows_x, 2 * block), jnp.bfloat16),
            pltpu.VMEM((rows_y, 2 * block), jnp.bfloat16),
            pltpu.VMEM((4 * depth * rows_x, rows_y), f32),
        ],
        name="backward",
    )(voxel_grid, pixel, start, count, target, x_low, x_high, part, *others)
    square_sum = global_sum(square)[0, 0]
    norm_value = jnp.sqrt(square_sum)
    limit = CLIP_RMS * math.sqrt(4.0 * total_depth * total_x * rows_y)
    clipped = gradient * (limit / jnp.maximum(norm_value, limit))
    new_first = BETA_ONE * first_moment + (1.0 - BETA_ONE) * clipped
    new_second = BETA_TWO * second_moment + (1.0 - BETA_TWO) * clipped * clipped
    first_hat = new_first / (1.0 - BETA_ONE**STEP)
    second_hat = new_second / (1.0 - BETA_TWO**STEP)
    new_grid = voxel_grid - LEARN_RATE * first_hat / (jnp.sqrt(second_hat) + EPSILON)
    return (new_grid, new_first, new_second)


def solution(mesh):
    placed = (
        P(None, "slab", "tile", None),
        P(None, "slab", "tile", None),
        P(None, "slab", "tile", None),
        P("tile"),
        P("tile"),
        P("tile"),
        P(None, "tile"),
    )
    return jax.shard_map(
        per_device,
        mesh=mesh,
        in_specs=placed,
        out_specs=(
            P(None, "slab", "tile", None),
            P(None, "slab", "tile", None),
            P(None, "slab", "tile", None),
        ),
        check_vma=False,
    )
```

```python
import math

import jax
import jax.numpy as jnp
from jax import lax
from jax.experimental import pallas as pl
from jax.experimental.pallas import tpu as pltpu
from jax.sharding import PartitionSpec as P


STEP = 20


RENDER_WEIGHT = 1000.0
TV_WEIGHT = 0.05
BACKGROUND = 1.0
STEP_SPAN = 4.0
CLIP_RMS = 0.25
LEARN_RATE = 0.02
BETA_ONE = 0.9
BETA_TWO = 0.99
EPSILON = 1e-08


def split_bf16(value):
    high = value.astype(jnp.bfloat16)
    low = (value - high.astype(jnp.float32)).astype(jnp.bfloat16)
    return high, low


def softplus(value):
    return jnp.maximum(value, 0.0) + jnp.log1p(jnp.exp(-jnp.abs(value)))


def ray_keys(pixel, start, count, slab_pos, depth, rows_x, rows_y):
    shift = rows_y.bit_length() - 1
    x = jnp.right_shift(pixel, shift)
    y = jnp.bitwise_and(pixel, rows_y - 1)
    first = (start - slab_pos) * depth
    used = jnp.clip(first + count, 0, depth)
    key = jnp.where((first <= 0) & (used > 0), (used - 1) * rows_x + x, -1)
    return y, key


def one_hot(y, rows_y):
    ids = lax.broadcasted_iota(jnp.int32, (rows_y, y.shape[1]), 0)
    return jnp.where(ids == y, 1.0, 0.0).astype(jnp.bfloat16)


def table_kernel(
    total_depth, grid, pixel, start, count, table, first_rows, last_rows, column, key
):
    channels, depth, rows_x, rows_y = grid.shape
    rows = depth * rows_x
    column[...], key[...] = ray_keys(
        pixel[...], start[...], count[...], lax.axis_index("slab"), depth, rows_x, rows_y
    )
    for c in range(channels):
        for z in range(depth):
            at = c * depth + z
            first_rows[at : at + 1] = grid[c, z, 0:1]
            last_rows[at : at + 1] = grid[c, z, rows_x - 1 : rows_x]
    reach = jnp.ones((rows_x, rows_y), jnp.float32)
    sums = [jnp.zeros((rows_x, rows_y), jnp.float32) for _ in range(3)]
    held = []
    for z in range(depth):
        fade = jnp.exp(-softplus(grid[0, z]) * (STEP_SPAN / total_depth))
        weight = reach * (1.0 - fade)
        reach = reach * fade
        sums = [sums[c] + weight * lax.logistic(grid[c + 1, z]) for c in range(3)]
        held.append(sums + [reach])
        if z % 2:
            for c in range(4):
                high, low = split_bf16(jnp.concatenate([held[0][c], held[1][c]], axis=0))
                at = c * rows + (z - 1) * rows_x
                table[at : at + 2 * rows_x, :rows_y] = high
                table[at : at + 2 * rows_x, rows_y:] = low
            held = []


def forward_kernel(grid, table, column, keys, part, to_next, to_prev):
    channels, depth, rows_x, rows_y = grid.shape
    rows = depth * rows_x
    rays = keys.shape[1]
    half = rays // 2
    block = math.gcd(half, 512)
    for at in range(0, rays, block):
        where = slice(at, at + block)
        y, key = column[:, where], keys[:, where]
        hot = one_hot(y, rows_y)
        picked = jnp.dot(
            table[...], jnp.concatenate([hot, hot], axis=0), preferred_element_type=jnp.float32
        )
        match = lax.broadcasted_iota(jnp.int32, (rows, block), 0) == key
        found = [
            jnp.sum(
                jnp.where(match, picked[c * rows : (c + 1) * rows], 0.0), axis=0, keepdims=True
            )
            for c in range(4)
        ]
        found[3] = jnp.where(key < 0, 1.0, found[3])
        found = jnp.concatenate(found, axis=0)
        row = 4 * (at // half)
        lane = at % half
        for out in (part, to_next, to_prev):
            out[row : row + 4, lane : lane + block] = found
    for c in range(channels):
        at = half + c * rows_y
        to_next[:, at : at + rows_y] = grid[c, depth - 1]
        to_prev[:, at : at + rows_y] = grid[c, 0]


def backward_kernel(
    slab_count, tile_count, grid, column, keys, target, x_low, x_high, part, *rest
):
    others = rest[: slab_count - 1]
    gradient, square, left, right, spread = rest[slab_count - 1 :]
    _, depth, rows_x, rows_y = grid.shape
    rows = depth * rows_x
    rays = keys.shape[1]
    half = rays // 2
    total_depth = depth * slab_count
    slab_pos = lax.axis_index("slab")
    tile_pos = lax.axis_index("tile")
    block = math.gcd(half, 1024)
    for at in range(0, rays, block):
        where = slice(at, at + block)
        row = 4 * (at // half)
        lanes = slice(at % half, at % half + block)

        def piece(ref):
            return ref[row : row + 3, lanes], ref[row + 3 : row + 4, lanes]

        front_color = jnp.zeros((3, block), jnp.float32)
        front_trans = jnp.ones((1, block), jnp.float32)
        beyond = jnp.full((3, block), BACKGROUND, jnp.float32)
        for k in range(slab_count - 1, 0, -1):
            color, trans = piece(others[k - 1])
            nearer = slab_pos >= k
            front_color = jnp.where(nearer, front_color + front_trans * color, front_color)
            front_trans = jnp.where(nearer, front_trans * trans, front_trans)
            color, trans = piece(others[slab_count - k - 1])
            farther = slab_pos + k < slab_count
            beyond = jnp.where(farther, color + trans * beyond, beyond)
        own_color, own_trans = piece(part)
        rendered = front_color + front_trans * (own_color + own_trans * beyond)
        residual = RENDER_WEIGHT * (rendered - target[:, where])
        color_cot = front_trans * residual
        trans_cot = front_trans * jnp.sum(residual * beyond, axis=0, keepdims=True)
        y, key = column[:, where], keys[:, where]
        hot = one_hot(y, rows_y)
        match = lax.broadcasted_iota(jnp.int32, (rows, block), 0) == key
        for c in range(4):
            cot = color_cot[c : c + 1] if c < 3 else trans_cot
            high = cot.astype(jnp.bfloat16).astype(jnp.float32)
            low = cot - high
            for j, value in enumerate((high, low)):
                left[c * rows : (c + 1) * rows, j * block : (j + 1) * block] = jnp.where(
                    match, value, 0.0
                ).astype(jnp.bfloat16)
        for j in range(2):
            right[:, j * block : (j + 1) * block] = hot
        added = lax.dot_general(
            left[...], right[...], (((1,), (1,)), ((), ())), preferred_element_type=jnp.float32
        )
        if at == 0:
            spread[...] = added
        else:
            spread[...] += added

    reach = [jnp.ones((rows_x, rows_y), jnp.float32)]
    fades = []
    for z in range(depth):
        fades.append(jnp.exp(-softplus(grid[0, z]) * (STEP_SPAN / total_depth)))
        reach.append(reach[z] * fades[z])
    row_ids = lax.broadcasted_iota(jnp.int32, (rows_x, rows_y), 0)
    lane_ids = lax.broadcasted_iota(jnp.int32, (rows_x, rows_y), 1)
    has_low = (row_ids > 0) | (tile_pos > 0)
    has_high = (row_ids < rows_x - 1) | (tile_pos < tile_count - 1)
    total = jnp.zeros((rows_x, rows_y), jnp.float32)

    def smooth(c, z):
        value = grid[c, z]
        lanes = slice(half + c * rows_y, half + (c + 1) * rows_y)
        if z > 0:
            out = value - grid[c, z - 1]
        else:
            out = jnp.where(slab_pos > 0, value - others[0][:, lanes], 0.0)
        if z < depth - 1:
            out = out + (value - grid[c, z + 1])
        else:
            out = out + jnp.where(
                slab_pos < slab_count - 1, value - others[slab_count - 2][:, lanes], 0.0
            )
        at = c * depth + z
        low = jnp.where(row_ids == 0, x_low[at : at + 1], pltpu.roll(value, 1, 0))
        high = jnp.where(
            row_ids == rows_x - 1, x_high[at : at + 1], pltpu.roll(value, rows_x - 1, 0)
        )
        out = out + jnp.where(has_low, value - low, 0.0) + jnp.where(has_high, value - high, 0.0)
        out = out + jnp.where(lane_ids > 0, value - pltpu.roll(value, 1, 1), 0.0)
        out = out + jnp.where(
            lane_ids < rows_y - 1, value - pltpu.roll(value, rows_y - 1, 1), 0.0
        )
        return (2.0 * TV_WEIGHT) * out

    below = [jnp.zeros((rows_x, rows_y), jnp.float32) for _ in range(3)]
    gain_after = jnp.zeros((rows_x, rows_y), jnp.float32)
    tail = jnp.zeros((rows_x, rows_y), jnp.float32)
    for z in range(depth - 1, -1, -1):
        rate = 1.0 - fades[z]
        weight = reach[z] * rate
        gain = jnp.zeros((rows_x, rows_y), jnp.float32)
        for c in range(3):
            at = c * rows + z * rows_x
            below[c] = below[c] + spread[at : at + rows_x]
            shade = lax.logistic(grid[c + 1, z])
            gain = gain + shade * below[c]
            value = weight * below[c] * shade * (1.0 - shade) + smooth(c + 1, z)
            gradient[c + 1, z] = value
            total = total + value * value
        at = 3 * rows + z * rows_x
        tail = tail + reach[z + 1] * (gain_after - gain + spread[at : at + rows_x])
        value = smooth(0, z) - tail * (STEP_SPAN / total_depth) * lax.logistic(grid[0, z])
        gradient[0, z] = value
        total = total + value * value
        gain_after = gain
    square[...] = jnp.broadcast_to(jnp.sum(total).reshape(1, 1), square.shape)


def global_sum(value):
    axes = ("slab", "tile")
    sent = jnp.broadcast_to(value[None], (lax.axis_size(axes),) + value.shape)
    return jnp.sum(lax.all_to_all(sent, axes, 0, 0), axis=0)


def whole_specs(count):
    return [pl.BlockSpec(memory_space=pltpu.VMEM) for _ in range(count)]


def in_vmem(*arrays):
    return [pltpu.with_memory_space_constraint(a, pltpu.VMEM) for a in arrays]


def per_device(voxel_grid, first_moment, second_moment, pixel_index, start_slab, ray_count, target):
    slab_count = lax.axis_size("slab")
    tile_count = lax.axis_size("tile")
    channels, depth, rows_x, rows_y = voxel_grid.shape
    total_depth = depth * slab_count
    total_x = rows_x * tile_count
    rays = pixel_index.shape[0]
    half = rays // 2
    f32 = jnp.float32
    pixel = pixel_index.reshape(1, rays)
    start = start_slab.reshape(1, rays)
    count = ray_count.reshape(1, rays)
    entries = 4 * depth * rows_x
    border = pltpu.VMEM((channels * depth, rows_y), f32)
    per_ray = pltpu.VMEM((1, rays), jnp.int32)
    table, first_rows, last_rows, column, key = pl.pallas_call(
        lambda *refs: table_kernel(total_depth, *refs),
        out_shape=(pltpu.VMEM((entries, 2 * rows_y), jnp.bfloat16), border, border, per_ray, per_ray),
        name="tables",
    )(voxel_grid, pixel, start, count)
    x_low = lax.ppermute(last_rows, "tile", [(i, i + 1) for i in range(tile_count - 1)])
    x_high = lax.ppermute(first_rows, "tile", [(i + 1, i) for i in range(tile_count - 1)])
    wide = pltpu.VMEM((8, half + channels * rows_y), f32)
    cost = pl.CostEstimate(
        flops=4 * entries * rows_y * rays, bytes_accessed=4 * voxel_grid.size, transcendentals=0
    )
    part, to_next, to_prev = pl.pallas_call(
        forward_kernel,
        in_specs=whole_specs(4),
        out_shape=(pltpu.VMEM((8, half), f32), wide, wide),
        cost_estimate=cost,
        name="forward",
    )(*in_vmem(voxel_grid, table, column, key))
    others = []
    for k in range(1, slab_count):
        sent = to_next if k == 1 else to_prev if k == slab_count - 1 else part
        others.append(
            lax.ppermute(sent, "slab", [(i, (i + k) % slab_count) for i in range(slab_count)])
        )
    block = math.gcd(half, 1024)
    gradient, square = pl.pallas_call(
        lambda *refs: backward_kernel(slab_count, tile_count, *refs),
        out_shape=(pltpu.VMEM(voxel_grid.shape, f32), pltpu.VMEM((1, 128), f32)),
        in_specs=whole_specs(6 + slab_count),
        cost_estimate=cost,
        scratch_shapes=[
            pltpu.VMEM((4 * depth * rows_x, 2 * block), jnp.bfloat16),
            pltpu.VMEM((rows_y, 2 * block), jnp.bfloat16),
            pltpu.VMEM((4 * depth * rows_x, rows_y), f32),
        ],
        name="backward",
    )(*in_vmem(voxel_grid, column, key, target, x_low, x_high, part, *others))
    square_sum = global_sum(square)[0, 0]
    norm_value = jnp.sqrt(square_sum)
    limit = CLIP_RMS * math.sqrt(4.0 * total_depth * total_x * rows_y)
    clipped = gradient * (limit / jnp.maximum(norm_value, limit))
    new_first = BETA_ONE * first_moment + (1.0 - BETA_ONE) * clipped
    new_second = BETA_TWO * second_moment + (1.0 - BETA_TWO) * clipped * clipped
    first_hat = new_first / (1.0 - BETA_ONE**STEP)
    second_hat = new_second / (1.0 - BETA_TWO**STEP)
    new_grid = voxel_grid - LEARN_RATE * first_hat / (jnp.sqrt(second_hat) + EPSILON)
    return (new_grid, new_first, new_second)


def solution(mesh):
    placed = (
        P(None, "slab", "tile", None),
        P(None, "slab", "tile", None),
        P(None, "slab", "tile", None),
        P("tile"),
        P("tile"),
        P("tile"),
        P(None, "tile"),
    )
    return jax.shard_map(
        per_device,
        mesh=mesh,
        in_specs=placed,
        out_specs=(
            P(None, "slab", "tile", None),
            P(None, "slab", "tile", None),
            P(None, "slab", "tile", None),
        ),
        check_vma=False,
    )
```
